32 devices in a mesh: site: 2 (over y), rows: 8 (over z, core), width: 2 (over x).
Axes of the slice: x: 2, y: 2, z: 4, core: 2. Of those that a mesh axis runs over, the one named last changes fastest.
Arguments:
- one_query: float32 [14336, 7168], P(('site', 'rows'), 'width'), parts along dimension 0, may hold values from -0.09375 to 0.09375
- other_query: float32 [14336, 7168], P(('site', 'rows'), 'width'), parts along dimension 0, may hold values from -0.0625 to 0.0625
- one_key: float32 [14336, 1024], P(('site', 'rows'), 'width'), parts along dimension 0, may hold values from -0.09375 to 0.09375
- other_key: float32 [14336, 1024], P(('site', 'rows'), 'width'), parts along dimension 0, may hold values from -0.0625 to 0.0625
- one_value: float32 [14336, 1024], P(('site', 'rows'), 'width'), parts along dimension 0, may hold values from -0.09375 to 0.09375
- other_value: float32 [14336, 1024], P(('site', 'rows'), 'width'), parts along dimension 0, may hold values from -0.0625 to 0.0625
- mix_share: float32 [14336], P(('site', 'rows')), parts along dimension 0, may hold values from 0.2 to 0.8
- norm_train: float32 [14336], P(('site', 'rows', 'width')), parts along dimension 0, may hold values from 0.25 to 1.75
- norm_step: float32 [14336], P(('site', 'rows', 'width')), parts along dimension 0, may hold values from -0.3 to 0.3
Outputs:
- serving_query: bfloat16 [14336, 7168], P('site', 'width'), parts along dimension 0
- serving_key: bfloat16 [14336, 1024], P('site', 'width'), parts along dimension 0
- serving_value: bfloat16 [14336, 1024], P('site', 'width'), parts along dimension 0
- scale_query: float32 [14336], P(('site', 'width')), parts along dimension 0
- scale_key: float32 [2048], P(('site', 'width')), parts along dimension 0
- scale_value: float32 [2048], P(('site', 'width')), parts along dimension 0
- serve_norm: bfloat16 [14336], P('site'), parts along dimension 0
The draws below stay inside these ranges and needn't reach their ends.
There are 2 independent parts, one for each index of `site`. The reference program is written for one: setup_inputs(seed, part) draws one part's arguments, and reference() takes and returns one part's arrays. A program takes and returns all parts, laid end to end along the dimension named above; each array names one. Nothing has to cross between parts.
All inputs are finite; a program needn't handle non-finite values. Where the reference program divides by a largest or mean magnitude, that divisor is 1e-20 or more.
Results may differ from the reference program's by a relative error of at most 0.001.
Values may be sent and summed in bfloat16 or wider, within the bound.
A program may use at most 256 MiB of HBM per device.

```python
import jax
import jax.numpy as jnp

D_MODEL = 7168
Q_DIM = 7168
KV_DIM = 1024


def raised(drawn, rng, source, target, blocks, factor):
    def block_of(dim):
        return (jnp.arange(drawn.shape[dim]) // (drawn.shape[dim] // blocks)).reshape((-1,) + (1,) * (drawn.ndim - 1 - dim))

    first = jax.random.permutation(rng, blocks)[block_of(target)]
    other_side = (block_of(target) + blocks // 2) % blocks
    return jnp.where((block_of(source) == first) | (block_of(source) == other_side), factor * drawn, drawn)


def level_of(own_key, dims, cuts, least, largest):
    loudness = 1.0
    for position, blocks in cuts:
        heights = jax.random.uniform(jax.random.fold_in(jax.random.fold_in(own_key, 6), position), (blocks,), jnp.float32, least / len(cuts), largest / len(cuts))
        loudness = loudness * jnp.repeat(jnp.exp(heights), dims[position] // blocks).reshape((-1,) + (1,) * (len(dims) - 1 - position))
    return loudness


def gaussian(stream_key, shape, width, most, shards=(), kind=jnp.bfloat16):
    result = jax.random.normal(stream_key, shape, jnp.float32) * width
    if len(shards) > 0:
        result = level_of(stream_key, shape, shards, -0.22, 0.18) * result
    return jnp.clip(result, min=-most, max=most).astype(kind)


def bell_draw_with(stream_key, extent, spread, reach, cuts, heavy, dtype=jnp.bfloat16):
    result = spread * jax.random.normal(stream_key, extent, jnp.float32)
    if cuts:
        result = result * level_of(stream_key, extent, cuts, -0.22, 0.18)
    return jnp.clip(raised(result, jax.random.fold_in(stream_key, 3), *heavy), -reach, reach).astype(dtype)


def setup_inputs(seed: int = 0, part: int = 0) -> dict:
    seeds = jax.random.split(jax.random.key(seed), 10)
    part_splits = jax.random.split(jax.random.fold_in(seeds[9], part), 10)
    return {
        "one_query": bell_draw_with(part_splits[0], (D_MODEL, Q_DIM), D_MODEL ** -0.5, 0.09375, ((0, 8), (1, 2)), (0, 1, 8, 2.0), jnp.float32),
        "other_query": gaussian(part_splits[1], (D_MODEL, Q_DIM), D_MODEL ** -0.5, 0.0625, ((0, 8), (1, 2)), jnp.float32),
        "one_key": bell_draw_with(part_splits[2], (D_MODEL, KV_DIM), D_MODEL ** -0.5, 0.09375, ((0, 8), (1, 2)), (0, 1, 8, 2.0), jnp.float32),
        "other_key": gaussian(part_splits[3], (D_MODEL, KV_DIM), D_MODEL ** -0.5, 0.0625, ((0, 8), (1, 2)), jnp.float32),
        "one_value": bell_draw_with(part_splits[4], (D_MODEL, KV_DIM), D_MODEL ** -0.5, 0.09375, ((0, 8), (1, 2)), (0, 1, 8, 2.0), jnp.float32),
        "other_value": gaussian(part_splits[5], (D_MODEL, KV_DIM), D_MODEL ** -0.5, 0.0625, ((0, 8), (1, 2)), jnp.float32),
        "mix_share": jnp.clip(0.2 + 0.6 * jax.random.uniform(part_splits[6], (D_MODEL,), jnp.float32) ** level_of(part_splits[6], (D_MODEL,), ((0, 8),), -0.2, 0.2), 0.2, 0.8),
        "norm_train": jnp.clip(1.0 + 0.15 * jax.random.normal(part_splits[7], (D_MODEL,), jnp.float32), 0.25, 1.75),
        "norm_step": jnp.clip(jax.random.uniform(part_splits[8], (D_MODEL,), jnp.float32, -0.3, 0.3) * level_of(part_splits[8], (D_MODEL,), ((0, 16),), -0.4, 0.0), -0.3, 0.3),
    }


def reference(one_query, other_query, one_key, other_key, one_value, other_value, mix_share, norm_train, norm_step):
    whole_query = mix_share[:, None] * one_query + (1.0 - mix_share[:, None]) * other_query
    whole_key = mix_share[:, None] * one_key + (1.0 - mix_share[:, None]) * other_key
    whole_value = mix_share[:, None] * one_value + (1.0 - mix_share[:, None]) * other_value
    scale_query = jnp.max(jnp.abs(whole_query), axis=0)
    serving_query = (whole_query / scale_query).astype(jnp.bfloat16)
    scale_key = jnp.max(jnp.abs(whole_key), axis=0)
    serving_key = (whole_key / scale_key).astype(jnp.bfloat16)
    scale_value = jnp.max(jnp.abs(whole_value), axis=0)
    serving_value = (whole_value / scale_value).astype(jnp.bfloat16)
    serve_norm = (norm_train + norm_step).astype(jnp.bfloat16)
    return serving_query, serving_key, serving_value, scale_query, scale_key, scale_value, serve_norm
```

```python
import functools

import jax
import jax.numpy as jnp
from jax import lax
from jax.experimental import pallas as pl
from jax.experimental.pallas import tpu as pltpu
from jax.sharding import PartitionSpec as P

MESH = pl.DeviceIdType.MESH
CORES = 2


def merge(
    ranks,
    widths,
    one_query,
    other_query,
    one_key,
    other_key,
    one_value,
    other_value,
    mix,
    norm_train,
    norm_step,
    query,
    key,
    value,
    scale_query,
    scale_key,
    scale_value,
    norms,
    one,
    other,
    narrow,
    peaks,
    load_sem,
    out_sem,
    peak_send,
    peak_recv,
    norm_send,
    norm_recv,
    up_send,
    up_recv,
    down_send,
    down_recv,
    side_send,
    side_recv,
):
    depth, span = one_key.shape
    parts = one_query.shape[1] // span
    chips = ranks // CORES
    me = lax.axis_index("rows")
    across = lax.axis_index("width")
    chip, core = me // CORES, me % CORES
    partner = chip * CORES + 1 - core
    group = ranks * widths
    block = 32 if depth % 32 == 0 else depth

    def loads(k):
        if isinstance(k, int) and k >= parts:
            sources = (one_key, other_key) if k == parts else (one_value, other_value)
        else:
            cut = pl.ds(pl.multiple_of(k * span, span), span)
            sources = one_query.at[:, cut], other_query.at[:, cut]
        return [
            pltpu.make_async_copy(source, target.at[k], load_sem.at[i, k])
            for i, (source, target) in enumerate(zip(sources, (one, other)))
        ]

    def each_part(body):
        pl.loop(0, parts)(body)

    @each_part
    def _(k):
        for copy in loads(k):
            copy.start()

    for k in (parts, parts + 1):
        for copy in loads(k):
            copy.start()

    barrier = pltpu.get_barrier_semaphore()
    mine = me * widths + across

    @pl.loop(1, group)
    def _(step):
        to = lax.rem(mine + step, group)
        pl.semaphore_signal(
            barrier,
            inc=1,
            device_id={"rows": to // widths, "width": lax.rem(to, widths)},
            device_id_type=MESH,
        )

    norms[mine] = norm_train[...] + norm_step[...]
    pl.semaphore_wait(barrier, group - 1)

    @pl.loop(1, group)
    def _(step):
        to = lax.rem(mine + step, group)
        pltpu.make_async_remote_copy(
            src_ref=norms.at[mine],
            dst_ref=norms.at[mine],
            send_sem=norm_send,
            recv_sem=norm_recv,
            device_id={"rows": to // widths, "width": lax.rem(to, widths)},
            device_id_type=MESH,
        ).start()

    def mixed(k):
        for copy in loads(k):
            copy.wait()

        def step(b, top):
            rows = pl.ds(pl.multiple_of(b * block, block), block)
            share = mix[rows]
            whole = share * one[k, rows] + (1.0 - share) * other[k, rows]
            one[k, rows] = whole
            return jnp.maximum(top, jnp.max(jnp.abs(whole).reshape(-1, 8, span), axis=0))

        top = lax.fori_loop(0, depth // block, step, jnp.zeros((8, span), jnp.float32))
        peaks[k, me] = jnp.max(top, axis=0, keepdims=True)

        @pl.loop(1, ranks)
        def _(step):
            pltpu.make_async_remote_copy(
                src_ref=peaks.at[k, me],
                dst_ref=peaks.at[k, me],
                send_sem=peak_send.at[k],
                recv_sem=peak_recv.at[k],
                device_id={"rows": lax.rem(me + step, ranks)},
                device_id_type=MESH,
            ).start()

    def slot(k, rank):
        rows = pl.ds(pl.multiple_of(rank * depth, depth), depth)
        if isinstance(k, int) and k == parts:
            return key.at[rows]
        return query.at[rows, pl.ds(pl.multiple_of(k * span, span), span)]

    def send(k, rank, to, send_sem, recv_sem):
        return pltpu.make_async_remote_copy(
            src_ref=slot(k, rank),
            dst_ref=slot(k, rank),
            send_sem=send_sem,
            recv_sem=recv_sem,
            device_id={"rows": to},
            device_id_type=MESH,
        )

    def go_up(k, hop):
        return send(k, me - CORES * hop, me + CORES, up_send.at[hop, k], up_recv.at[hop, k])

    def go_down(k, hop):
        return send(k, me + CORES * hop, me - CORES, down_send.at[hop, k], down_recv.at[hop, k])

    def go_side(k, hop):
        index = hop + chips - 1
        return send(k, me + CORES * hop, partner, side_send.at[index, k], side_recv.at[index, k])

    def from_side(k, hop):
        index = hop + chips - 1
        return send(
            k, partner + CORES * hop, partner, side_send.at[index, k], side_recv.at[index, k]
        )

    def from_below(k, hop):
        return send(k, me - CORES * (hop + 1), me - CORES, up_send.at[hop, k], up_recv.at[hop, k])

    def from_above(k, hop):
        return send(
            k, me + CORES * (hop + 1), me + CORES, down_send.at[hop, k], down_recv.at[hop, k]
        )

    has_below, has_above = chip >= 1, chip < chips - 1

    def scaled(k, scale_ref, cut):
        everyone = peaks.at[k, pl.ds(0, ranks - 1)]
        pltpu.make_async_copy(everyone, everyone, peak_recv.at[k]).wait()
        scale = jnp.max(peaks[k], axis=0)
        scale_ref[:, cut] = scale

        @pl.loop(0, depth // block)
        def _(b):
            rows = pl.ds(pl.multiple_of(b * block, block), block)
            narrow[k, rows] = (one[k, rows] / scale).astype(jnp.bfloat16)

        target = value if isinstance(k, int) and k > parts else slot(k, me)
        copy = pltpu.make_async_copy(narrow.at[k], target, out_sem.at[k])
        copy.start()
        if isinstance(k, int) and k > parts:
            copy.wait()
            return
        copy.wait()

        @pl.when(has_above)
        def _():
            go_up(k, 0).start()

        @pl.when(has_below)
        def _():
            go_down(k, 0).start()

        go_side(k, 0).start()

    lag = min(2, parts)
    pl.loop(0, lag)(mixed)

    def part_cut(k):
        return pl.ds(pl.multiple_of(k * span, span), span)

    @pl.loop(0, parts - lag)
    def _(k):
        mixed(k + lag)
        scaled(k, scale_query, part_cut(k))

    mixed(parts)
    mixed(parts + 1)

    @pl.loop(parts - lag, parts)
    def _(k):
        scaled(k, scale_query, part_cut(k))

    scaled(parts, scale_key, slice(None))
    scaled(parts + 1, scale_value, slice(None))

    def relay(k, hop):
        @pl.when(chip >= hop)
        def _():
            from_below(k, hop - 1).wait_recv()

            @pl.when(has_above)
            def _():
                go_up(k, hop).start()

            go_side(k, -hop).start()

        @pl.when(chip + hop < chips)
        def _():
            from_above(k, hop - 1).wait_recv()

            @pl.when(has_below)
            def _():
                go_down(k, hop).start()

            go_side(k, hop).start()

    @pl.loop(1, chips)
    def _(hop):
        each_part(lambda k: relay(k, hop))
        relay(parts, hop)

    def finish(k):
        @pl.loop(0, chips - 1)
        def _(hop):
            @pl.when((chip >= hop) & has_above)
            def _():
                go_up(k, hop).wait_send()

            @pl.when((chip + hop < chips) & has_below)
            def _():
                go_down(k, hop).wait_send()

        @pl.loop(0, chips)
        def _(origin):
            go_side(k, origin - chip).wait_send()
            from_side(k, origin - chip).wait_recv()

    each_part(finish)
    finish(parts)

    def settle(k):
        everyone = peaks.at[k, pl.ds(0, ranks - 1)]
        pltpu.make_async_copy(everyone, everyone, peak_send.at[k]).wait()

    pl.loop(0, parts + 2)(settle)
    others = norms.at[pl.ds(0, group - 1)]
    pltpu.make_async_copy(others, others, norm_recv).wait()
    pltpu.make_async_copy(others, others, norm_send).wait()


def shards(
    ranks,
    widths,
    one_query,
    other_query,
    one_key,
    other_key,
    one_value,
    other_value,
    mix_share,
    norm_train,
    norm_step,
):
    depth, span = one_key.shape
    wide = one_query.shape[1]
    parts = wide // span
    chips = ranks // CORES
    group = ranks * widths
    bit = norm_train.shape[0]
    shape = jax.ShapeDtypeStruct
    anywhere = pl.BlockSpec(memory_space=pl.ANY)
    near = pl.BlockSpec(memory_space=pltpu.VMEM)
    dma = pltpu.SemaphoreType.DMA
    query, key, value, scale_query, scale_key, scale_value, norms = pl.pallas_call(
        functools.partial(merge, ranks, widths),
        out_shape=(
            shape((ranks * depth, wide), jnp.bfloat16),
            shape((ranks * depth, span), jnp.bfloat16),
            shape((depth, span), jnp.bfloat16),
            shape((1, wide), jnp.float32),
            shape((1, span), jnp.float32),
            shape((1, span), jnp.float32),
            shape((group, 1, bit), jnp.float32),
        ),
        in_specs=[anywhere] * 6 + [near] * 3,
        out_specs=[anywhere] * 3 + [near] * 4,
        scratch_shapes=[
            pltpu.VMEM((parts + 2, depth, span), jnp.float32),
            pltpu.VMEM((parts + 2, depth, span), jnp.float32),
            pltpu.VMEM((parts + 2, depth, span), jnp.bfloat16),
            pltpu.VMEM((parts + 2, ranks, 1, span), jnp.float32),
            dma((2, parts + 2)),
            dma((parts + 2,)),
            dma((parts + 2,)),
            dma((parts + 2,)),
            dma,
            dma,
            dma((chips - 1, parts + 1)),
            dma((chips - 1, parts + 1)),
            dma((chips - 1, parts + 1)),
            dma((chips - 1, parts + 1)),
            dma((2 * chips - 1, parts + 1)),
            dma((2 * chips - 1, parts + 1)),
        ],
        compiler_params=pltpu.CompilerParams(
            collective_id=0, has_side_effects=True, vmem_limit_bytes=56 * 2**20
        ),
    )(
        one_query,
        other_query,
        one_key,
        other_key,
        one_value,
        other_value,
        mix_share[:, None],
        norm_train[None],
        norm_step[None],
    )
    value = lax.all_gather(value, "rows", axis=0, tiled=True)
    return (
        query,
        key,
        value,
        scale_query[0],
        scale_key[0],
        scale_value[0],
        norms.reshape(-1).astype(jnp.bfloat16),
    )


def solution(mesh):
    in_specs = (
        P(("site", "rows"), "width"),
        P(("site", "rows"), "width"),
        P(("site", "rows"), "width"),
        P(("site", "rows"), "width"),
        P(("site", "rows"), "width"),
        P(("site", "rows"), "width"),
        P(("site", "rows")),
        P(("site", "rows", "width")),
        P(("site", "rows", "width")),
    )
    out_specs = (
        P("site", "width"),
        P("site", "width"),
        P("site", "width"),
        P(("site", "width")),
        P(("site", "width")),
        P(("site", "width")),
        P("site"),
    )
    body = functools.partial(shards, mesh.shape["rows"], mesh.shape["width"])
    return jax.shard_map(body, mesh=mesh, in_specs=in_specs, out_specs=out_specs, check_vma=False)
```

```python
import functools

import jax
import jax.numpy as jnp
from jax import lax
from jax.experimental import pallas as pl
from jax.experimental.pallas import tpu as pltpu
from jax.sharding import PartitionSpec as P

MESH = pl.DeviceIdType.MESH
CORES = 2


def merge(
    ranks,
    widths,
    one_query,
    other_query,
    one_key,
    other_key,
    one_value,
    other_value,
    mix,
    norm_train,
    norm_step,
    query,
    key,
    value,
    scale_query,
    scale_key,
    scale_value,
    norms,
    one,
    other,
    narrow,
    peaks,
    load_sem,
    out_sem,
    peak_send,
    peak_recv,
    norm_send,
    norm_recv,
    up_send,
    up_recv,
    down_send,
    down_recv,
    side_send,
    side_recv,
):
    depth, span = one_key.shape
    parts = one_query.shape[1] // span
    chips = ranks // CORES
    me = lax.axis_index("rows")
    across = lax.axis_index("width")
    chip, core = me // CORES, me % CORES
    partner = chip * CORES + 1 - core
    group = ranks * widths
    block = 32 if depth % 32 == 0 else depth

    def loads(k):
        if isinstance(k, int) and k >= parts:
            sources = (one_key, other_key) if k == parts else (one_value, other_value)
        else:
            cut = pl.ds(pl.multiple_of(k * span, span), span)
            sources = one_query.at[:, cut], other_query.at[:, cut]
        return [
            pltpu.make_async_copy(source, target.at[k], load_sem.at[i, k])
            for i, (source, target) in enumerate(zip(sources, (one, other)))
        ]

    def each_part(body):
        pl.loop(0, parts)(body)

    @each_part
    def _(k):
        for copy in loads(k):
            copy.start()

    for k in (parts, parts + 1):
        for copy in loads(k):
            copy.start()

    barrier = pltpu.get_barrier_semaphore()
    mine = me * widths + across

    @pl.loop(1, group)
    def _(step):
        to = lax.rem(mine + step, group)
        pl.semaphore_signal(
            barrier,
            inc=1,
            device_id={"rows": to // widths, "width": lax.rem(to, widths)},
            device_id_type=MESH,
        )

    norms[mine] = norm_train[...] + norm_step[...]
    pl.semaphore_wait(barrier, group - 1)

    @pl.loop(1, group)
    def _(step):
        to = lax.rem(mine + step, group)
        pltpu.make_async_remote_copy(
            src_ref=norms.at[mine],
            dst_ref=norms.at[mine],
            send_sem=norm_send,
            recv_sem=norm_recv,
            device_id={"rows": to // widths, "width": lax.rem(to, widths)},
            device_id_type=MESH,
        ).start()

    def mixed(k):
        for copy in loads(k):
            copy.wait()

        def step(b, top):
            rows = pl.ds(pl.multiple_of(b * block, block), block)
            share = mix[rows]
            whole = share * one[k, rows] + (1.0 - share) * other[k, rows]
            one[k, rows] = whole
            return jnp.maximum(top, jnp.max(jnp.abs(whole).reshape(-1, 8, span), axis=0))

        top = lax.fori_loop(0, depth // block, step, jnp.zeros((8, span), jnp.float32))
        peaks[k, me] = jnp.max(top, axis=0, keepdims=True)

        @pl.loop(1, ranks)
        def _(step):
            pltpu.make_async_remote_copy(
                src_ref=peaks.at[k, me],
                dst_ref=peaks.at[k, me],
                send_sem=peak_send.at[k],
                recv_sem=peak_recv.at[k],
                device_id={"rows": lax.rem(me + step, ranks)},
                device_id_type=MESH,
            ).start()

    def is_tail(k):
        return isinstance(k, int) and k >= parts

    def hops(k):
        return chips - 2 if is_tail(k) else chips - 1

    def slot(k, rank):
        rows = pl.ds(pl.multiple_of(rank * depth, depth), depth)
        if is_tail(k):
            return (key if k == parts else value).at[rows]
        return query.at[rows, pl.ds(pl.multiple_of(k * span, span), span)]

    def send(k, rank, to, send_sem, recv_sem):
        return pltpu.make_async_remote_copy(
            src_ref=slot(k, rank),
            dst_ref=slot(k, rank),
            send_sem=send_sem,
            recv_sem=recv_sem,
            device_id={"rows": to},
            device_id_type=MESH,
        )

    def go_up(k, hop):
        return send(k, me - CORES * hop, me + CORES, up_send.at[hop, k], up_recv.at[hop, k])

    def go_down(k, hop):
        return send(k, me + CORES * hop, me - CORES, down_send.at[hop, k], down_recv.at[hop, k])

    def go_side(k, hop):
        index = hop + chips - 1
        return send(k, me + CORES * hop, partner, side_send.at[index, k], side_recv.at[index, k])

    def from_side(k, hop):
        index = hop + chips - 1
        return send(
            k, partner + CORES * hop, partner, side_send.at[index, k], side_recv.at[index, k]
        )

    def from_below(k, hop):
        return send(k, me - CORES * (hop + 1), me - CORES, up_send.at[hop, k], up_recv.at[hop, k])

    def from_above(k, hop):
        return send(
            k, me + CORES * (hop + 1), me + CORES, down_send.at[hop, k], down_recv.at[hop, k]
        )

    has_below, has_above = chip >= 1, chip < chips - 1

    def scaled(k, scale_ref, cut):
        everyone = peaks.at[k, pl.ds(0, ranks - 1)]
        pltpu.make_async_copy(everyone, everyone, peak_recv.at[k]).wait()
        scale = jnp.max(peaks[k], axis=0)
        scale_ref[:, cut] = scale

        @pl.loop(0, depth // block)
        def _(b):
            rows = pl.ds(pl.multiple_of(b * block, block), block)
            narrow[k, rows] = (one[k, rows] / scale).astype(jnp.bfloat16)

        copy = pltpu.make_async_copy(narrow.at[k], slot(k, me), out_sem.at[k])
        copy.start()
        copy.wait()

        if hops(k) > 0:

            @pl.when(has_above)
            def _():
                go_up(k, 0).start()

            @pl.when(has_below)
            def _():
                go_down(k, 0).start()

        go_side(k, 0).start()

    lag = min(2, parts)
    pl.loop(0, lag)(mixed)

    def part_cut(k):
        return pl.ds(pl.multiple_of(k * span, span), span)

    @pl.loop(0, parts - lag)
    def _(k):
        mixed(k + lag)
        scaled(k, scale_query, part_cut(k))

    mixed(parts)
    mixed(parts + 1)

    @pl.loop(parts - lag, parts)
    def _(k):
        scaled(k, scale_query, part_cut(k))

    scaled(parts, scale_key, slice(None))
    scaled(parts + 1, scale_value, slice(None))

    def relay(k, hop):
        onward = hop < hops(k)

        @pl.when(chip >= hop)
        def _():
            from_below(k, hop - 1).wait_recv()

            @pl.when(has_above & onward)
            def _():
                go_up(k, hop).start()

            go_side(k, -hop).start()

        @pl.when(chip + hop < chips)
        def _():
            from_above(k, hop - 1).wait_recv()

            @pl.when(has_below & onward)
            def _():
                go_down(k, hop).start()

            go_side(k, hop).start()

    @pl.loop(1, chips - 1)
    def _(hop):
        each_part(lambda k: relay(k, hop))
        relay(parts, hop)
        relay(parts + 1, hop)

    each_part(lambda k: relay(k, chips - 1))

    def finish(k):
        @pl.loop(0, hops(k))
        def _(hop):
            @pl.when((chip >= hop) & has_above)
            def _():
                go_up(k, hop).wait_send()

            @pl.when((chip + hop < chips) & has_below)
            def _():
                go_down(k, hop).wait_send()

        @pl.loop(0, chips)
        def _(origin):
            @pl.when((origin - chip <= hops(k)) & (chip - origin <= hops(k)))
            def _():
                go_side(k, origin - chip).wait_send()
                from_side(k, origin - chip).wait_recv()

    each_part(finish)
    finish(parts)
    finish(parts + 1)

    def settle(k):
        everyone = peaks.at[k, pl.ds(0, ranks - 1)]
        pltpu.make_async_copy(everyone, everyone, peak_send.at[k]).wait()

    pl.loop(0, parts + 2)(settle)
    others = norms.at[pl.ds(0, group - 1)]
    pltpu.make_async_copy(others, others, norm_recv).wait()
    pltpu.make_async_copy(others, others, norm_send).wait()


def settle_block(source, target, done):
    target[...] = source[...]
    done[...] = jnp.zeros_like(done)


def settled(whole, step):
    rows, wide = whole.shape
    spec = pl.BlockSpec((step, wide), lambda i: (i, 0))
    return pl.pallas_call(
        settle_block,
        out_shape=(
            jax.ShapeDtypeStruct(whole.shape, whole.dtype),
            jax.ShapeDtypeStruct((8, 128), jnp.float32),
        ),
        grid=(rows // step,),
        in_specs=[spec],
        out_specs=(spec, pl.BlockSpec((8, 128), lambda i: (0, 0))),
        cost_estimate=pl.CostEstimate(
            flops=0, bytes_accessed=4 * rows * wide, transcendentals=0
        ),
    )(whole)


def place_block(at, whole, got, side, target):
    i = pl.program_id(0)

    @pl.when(at[2] == 0)
    def _():
        target[...] = whole[...]

    @pl.when((at[2] == 1) & (i == 0))
    def _():
        target[...] = got[...]

    @pl.when((at[2] == 1) & (i == 1))
    def _():
        target[...] = side[...]


def placed(at, whole, got, side):
    depth, span = got.shape
    one = pl.BlockSpec((depth, span), lambda i, at: (0, 0))
    spec = pl.BlockSpec((depth, span), lambda i, at: (at[i], 0))
    return pl.pallas_call(
        place_block,
        out_shape=jax.ShapeDtypeStruct(whole.shape, whole.dtype),
        grid_spec=pltpu.PrefetchScalarGridSpec(
            num_scalar_prefetch=1, grid=(2,), in_specs=[spec, one, one], out_specs=spec
        ),
        input_output_aliases={1: 0},
        cost_estimate=pl.CostEstimate(
            flops=0, bytes_accessed=12 * depth * span, transcendentals=0
        ),
    )(at, whole, got, side)


def shards(
    ranks,
    widths,
    one_query,
    other_query,
    one_key,
    other_key,
    one_value,
    other_value,
    mix_share,
    norm_train,
    norm_step,
):
    depth, span = one_key.shape
    wide = one_query.shape[1]
    parts = wide // span
    chips = ranks // CORES
    group = ranks * widths
    bit = norm_train.shape[0]
    shape = jax.ShapeDtypeStruct
    anywhere = pl.BlockSpec(memory_space=pl.ANY)
    near = pl.BlockSpec(memory_space=pltpu.VMEM)
    dma = pltpu.SemaphoreType.DMA
    query, key, value, scale_query, scale_key, scale_value, norms = pl.pallas_call(
        functools.partial(merge, ranks, widths),
        out_shape=(
            shape((ranks * depth, wide), jnp.bfloat16),
            shape((ranks * depth, span), jnp.bfloat16),
            shape((ranks * depth, span), jnp.bfloat16),
            shape((1, wide), jnp.float32),
            shape((1, span), jnp.float32),
            shape((1, span), jnp.float32),
            shape((group, 1, bit), jnp.float32),
        ),
        in_specs=[anywhere] * 6 + [near] * 3,
        out_specs=[anywhere] * 3 + [near] * 4,
        scratch_shapes=[
            pltpu.VMEM((parts + 2, depth, span), jnp.float32),
            pltpu.VMEM((parts + 2, depth, span), jnp.float32),
            pltpu.VMEM((parts + 2, depth, span), jnp.bfloat16),
            pltpu.VMEM((parts + 2, ranks, 1, span), jnp.float32),
            dma((2, parts + 2)),
            dma((parts + 2,)),
            dma((parts + 2,)),
            dma((parts + 2,)),
            dma,
            dma,
            dma((chips - 1, parts + 2)),
            dma((chips - 1, parts + 2)),
            dma((chips - 1, parts + 2)),
            dma((chips - 1, parts + 2)),
            dma((2 * chips - 1, parts + 2)),
            dma((2 * chips - 1, parts + 2)),
        ],
        compiler_params=pltpu.CompilerParams(
            collective_id=0, has_side_effects=True, vmem_limit_bytes=56 * 2**20
        ),
    )(
        one_query,
        other_query,
        one_key,
        other_key,
        one_value,
        other_value,
        mix_share[:, None],
        norm_train[None],
        norm_step[None],
    )
    me = lax.axis_index("rows")
    chip, core = me // CORES, me % CORES
    far = jnp.where(chip == 1, chips - 1, 0) * CORES + core
    ends = (0, chips - 1)
    out = [
        (near * CORES + c, end * CORES + c)
        for near, end in ((1, 0), (chips - 2, chips - 1))
        for c in range(CORES)
    ]
    across = [(end * CORES + c, end * CORES + 1 - c) for end in ends for c in range(CORES)]

    def last_hop(whole):
        piece = lax.dynamic_slice_in_dim(whole, far * depth, depth, 0)
        return lax.ppermute(piece, "rows", out)

    from_key, from_value = last_hop(key), last_hop(value)
    query, query_done = settled(query, depth // 2 if depth % 32 == 0 else depth)
    key, key_done = settled(key, depth)
    value, value_done = settled(value, depth)
    done = query_done, key_done, value_done
    from_key, _ = lax.optimization_barrier((from_key, done))
    side_key = lax.ppermute(from_key, "rows", across)
    from_value, _ = lax.optimization_barrier((from_value, done))
    side_value = lax.ppermute(from_value, "rows", across)
    at_end = (chip == 0) | (chip == chips - 1)
    away = jnp.where(chip == 0, chips - 1, 0) * CORES
    at = jnp.stack([away + core, away + 1 - core, at_end.astype(jnp.int32)])
    return (
        query,
        placed(at, key, from_key, side_key),
        placed(at, value, from_value, side_value),
        scale_query[0],
        scale_key[0],
        scale_value[0],
        norms.reshape(-1).astype(jnp.bfloat16),
    )


def solution(mesh):
    in_specs = (
        P(("site", "rows"), "width"),
        P(("site", "rows"), "width"),
        P(("site", "rows"), "width"),
        P(("site", "rows"), "width"),
        P(("site", "rows"), "width"),
        P(("site", "rows"), "width"),
        P(("site", "rows")),
        P(("site", "rows", "width")),
        P(("site", "rows", "width")),
    )
    out_specs = (
        P("site", "width"),
        P("site", "width"),
        P("site", "width"),
        P(("site", "width")),
        P(("site", "width")),
        P(("site", "width")),
        P("site"),
    )
    body = functools.partial(shards, mesh.shape["rows"], mesh.shape["width"])
    return jax.shard_map(body, mesh=mesh, in_specs=in_specs, out_specs=out_specs, check_vma=False)
```
